32 devices in a mesh: stage: 4 (over z), data: 8 (over y, x, core).
Axes of the slice: x: 2, y: 2, z: 4, core: 2. Of those that a mesh axis runs over, the one named last changes fastest.
Arguments:
- tokens_in: bfloat16 [32, 64, 1536], P('data')
- targets: bfloat16 [32, 64, 1536], P('data')
- w_up: bfloat16 [4, 1536, 8960], P('stage')
- w_down: bfloat16 [4, 8960, 1536], P('stage')
- clip_norm: float32 [], replicated
Outputs:
- output 1: float32 [], replicated
- output 2: float32 [4, 1536, 8960], P('stage', 'data')
- output 3: float32 [4, 8960, 1536], P('stage', None, 'data')
All inputs are finite; a program needn't handle non-finite values.
Results may differ from the reference program's by a relative error of at most 0.00741393.
Values are sent between devices in bfloat16 or wider.
A program may use at most 1 GiB of HBM per device.

```python
import jax
import jax.numpy as jnp
from jax import lax

MODEL_DIM = 1536
FFN_DIM = 8960
MICRO_TOKENS = 64
MICRO_COUNT = 4
STAGE_LAYERS = 1
NUM_STAGES = 4
NUM_REPLICAS = 8

NUM_LAYERS = STAGE_LAYERS * NUM_STAGES
BATCH_ROWS = NUM_REPLICAS * MICRO_COUNT
TOTAL_TOKENS = BATCH_ROWS * MICRO_TOKENS


def layer_forward(hidden, w_up_l, w_down_l):
    up_val = jnp.dot(hidden, w_up_l, preferred_element_type=jnp.float32)
    gelu_out = jax.nn.gelu(up_val).astype(jnp.bfloat16)
    branch = jnp.dot(gelu_out, w_down_l, preferred_element_type=jnp.float32)
    return (hidden.astype(jnp.float32) + branch).astype(jnp.bfloat16)


def layer_backward(hidden, g_out, w_up_l, w_down_l):
    up_val = jnp.dot(hidden, w_up_l, preferred_element_type=jnp.float32)
    gelu_val, gelu_vjp = jax.vjp(jax.nn.gelu, up_val)
    gelu_out = gelu_val.astype(jnp.bfloat16)
    grad_down_l = jnp.dot(gelu_out.T, g_out, preferred_element_type=jnp.float32)
    grad_act = jnp.dot(g_out, w_down_l.T, preferred_element_type=jnp.float32)
    grad_pre = gelu_vjp(grad_act)[0].astype(jnp.bfloat16)
    grad_up_l = jnp.dot(hidden.T, grad_pre, preferred_element_type=jnp.float32)
    back_prop = jnp.dot(grad_pre, w_up_l.T, preferred_element_type=jnp.float32)
    g_in = (g_out.astype(jnp.float32) + back_prop).astype(jnp.bfloat16)
    return g_in, grad_up_l, grad_down_l


def micro_grads(tokens_mb, targets_mb, w_up, w_down):
    def fwd_step(hidden, weights):
        return layer_forward(hidden, weights[0], weights[1]), hidden

    h_top, h_saved = lax.scan(fwd_step, tokens_mb, (w_up, w_down))
    resid_err = h_top.astype(jnp.float32) - targets_mb.astype(jnp.float32)
    loss_part = jnp.sum(resid_err * resid_err) / (2 * TOTAL_TOKENS)
    g_top = (resid_err / TOTAL_TOKENS).astype(jnp.bfloat16)

    def bwd_step(g_cur, saved_all):
        g_in, grad_up_l, grad_down_l = layer_backward(saved_all[0], g_cur, saved_all[1], saved_all[2])
        return g_in, (grad_up_l, grad_down_l)

    unused_g, layer_grads = lax.scan(bwd_step, g_top, (h_saved, w_up, w_down), reverse=True)
    return loss_part, layer_grads[0], layer_grads[1]


def full_grads(tokens_in, targets, w_up, w_down):
    def micro_body(loop_state, batch_item):
        loss_part, grad_up_mb, grad_down_mb = micro_grads(batch_item[0], batch_item[1], w_up, w_down)
        return (loop_state[0] + loss_part, loop_state[1] + grad_up_mb, loop_state[2] + grad_down_mb), None

    init_state = (jnp.zeros((), jnp.float32), jnp.zeros(w_up.shape, jnp.float32), jnp.zeros(w_down.shape, jnp.float32))
    final_state, unused_out = lax.scan(micro_body, init_state, (tokens_in, targets))
    return final_state


def setup_inputs(seed: int = 0) -> dict:
    base_key = jax.random.key(seed)
    key_tokens, key_targets, key_up, key_down, key_clip = jax.random.split(base_key, 5)
    data_shape = (BATCH_ROWS, MICRO_TOKENS, MODEL_DIM)
    tokens_in = jax.random.normal(key_tokens, data_shape, jnp.float32).astype(jnp.bfloat16)
    targets = jax.random.normal(key_targets, data_shape, jnp.float32).astype(jnp.bfloat16)
    w_up = (jax.random.normal(key_up, (NUM_LAYERS, MODEL_DIM, FFN_DIM), jnp.float32) * MODEL_DIM ** -0.5).astype(jnp.bfloat16)
    w_down = (jax.random.normal(key_down, (NUM_LAYERS, FFN_DIM, MODEL_DIM), jnp.float32) * (FFN_DIM * NUM_LAYERS) ** -0.5).astype(jnp.bfloat16)
    unused_loss, grad_up, grad_down = full_grads(tokens_in, targets, w_up, w_down)
    grad_norm = jnp.sqrt(jnp.sum(grad_up * grad_up) + jnp.sum(grad_down * grad_down))
    clip_ratio = jax.random.uniform(key_clip, (), jnp.float32, 0.5, 0.85)
    clip_norm = (clip_ratio * grad_norm).astype(jnp.float32)
    return {"tokens_in": tokens_in, "targets": targets, "w_up": w_up, "w_down": w_down, "clip_norm": clip_norm}


def reference(tokens_in, targets, w_up, w_down, clip_norm):
    loss_total, grad_up, grad_down = full_grads(tokens_in, targets, w_up, w_down)
    norm_sq = jnp.sum(grad_up * grad_up) + jnp.sum(grad_down * grad_down)
    clip_scale = jnp.minimum(1.0, clip_norm / jnp.sqrt(norm_sq))
    return loss_total, grad_up * clip_scale, grad_down * clip_scale
```

```python
import functools

import jax
import jax.numpy as jnp
from jax import lax
from jax.experimental import pallas as pl
from jax.experimental.pallas import tpu as pltpu
from jax.sharding import PartitionSpec as P

F32 = jnp.float32
BF16 = jnp.bfloat16
MESH = pl.DeviceIdType.MESH
K0 = 0.7978845608028654
K1 = 0.044715


def mm(a, b, dims):
    return lax.dot_general(a, b, (dims, ((), ())), preferred_element_type=F32)


def gelu_grad(u):
    uu = u * u
    t = jnp.tanh(K0 * u * (1.0 + K1 * uu))
    return 0.5 * (1.0 + t) + (0.5 * K0) * u * (1.0 - t * t) * (1.0 + 3.0 * K1 * uu)


def gelu(u):
    t = jnp.tanh(K0 * (u + K1 * (u * u * u)))
    return (u * (0.5 * (1.0 + t))).astype(BF16)


def f_tiles(half):
    first = (half + 511) // 512 * 256
    return [(0, first), (first, half - first)]


def chain_kernel(n_stages, total, x_ref, y_ref, w1_ref, w2_ref, hall, gall, loss_ref,
                 w1, w2, hbuf, gbuf, ubuf, pf, pb, rf, rb, yv, hsend, gsend,
                 s_w, s_l, s_h, r_h, s_g, r_g, s_x, r_x, s_p, r_p, s_a, r_a, s_f, r_f):
    stage = lax.axis_index("stage")
    data = lax.axis_index("data")
    chip, core = data // 2, data % 2
    nc, rows2, dim = hbuf.shape
    rows = rows2 // 2
    half = w1.shape[1]
    nchip = hall.shape[0]
    partner = (stage, chip * 2 + (1 - core))
    last = n_stages - 1
    mine = pl.ds(pl.multiple_of(core * rows, rows), rows)
    theirs = pl.ds(pl.multiple_of((1 - core) * rows, rows), rows)
    foff = pl.multiple_of(core * half, 128)
    tiles = f_tiles(half)

    def rc(src, dst, ss, rs, dev):
        return pltpu.make_async_remote_copy(
            src_ref=src, dst_ref=dst, send_sem=ss, recv_sem=rs, device_id=dev, device_id_type=MESH)

    wcopies = [
        pltpu.make_async_copy(w1_ref.at[0, :, pl.ds(foff, half)], w1, s_w.at[0]),
        pltpu.make_async_copy(w2_ref.at[0, pl.ds(foff, half), :], w2, s_w.at[1]),
    ]

    @pl.when(stage == 0)
    def _():
        for j in range(nc):
            pltpu.make_async_copy(x_ref.at[j], hbuf.at[j, mine], s_l.at[j]).start()

    for c in wcopies:
        c.start()

    @pl.when(stage == last)
    def _():
        for j in range(nc):
            pltpu.make_async_copy(y_ref.at[j], yv.at[j], s_l.at[j]).start()

    @pl.when(stage == 0)
    def _():
        for j in range(nc):
            pltpu.make_async_copy(x_ref.at[j], hbuf.at[j, mine], s_l.at[j]).wait()

    @pl.when(stage == last)
    def _():
        for j in range(nc):
            pltpu.make_async_copy(y_ref.at[j], yv.at[j], s_l.at[j]).wait()

    loss_ref[...] = jnp.zeros_like(loss_ref)

    def share(kind, buf, j):
        return rc(buf.at[j, mine], buf.at[j, mine], s_x.at[kind, j], r_x.at[kind, j], partner)

    def spread(kind, buf, allr, j, o):
        other = (chip + o) % nchip
        return rc(buf.at[j, mine], allr.at[chip, j, mine], s_a.at[kind, j, o], r_a.at[kind, j, o],
                  (stage, other * 2 + core))

    def arrived(kind, buf, allr, j, o):
        src = (chip + nchip - o) % nchip
        return rc(buf.at[j, mine], allr.at[src, j, mine], s_a.at[kind, j, o], r_a.at[kind, j, o], partner)

    def forward(kind, allr, j, o):
        src = (chip + nchip - o) % nchip
        return rc(allr.at[src, j, mine], allr.at[src, j, mine], s_f.at[kind, j, o], r_f.at[kind, j, o], partner)

    def own(kind, buf, allr, j):
        return pltpu.make_async_copy(buf.at[j], allr.at[chip, j], s_f.at[kind, j, 0])

    def hand_up(j):
        return rc(hsend.at[j], hbuf.at[j, mine], s_h.at[j], r_h.at[j], (jnp.minimum(stage + 1, last), data))

    def hand_down(j):
        return rc(gsend.at[j], gbuf.at[j, mine], s_g.at[j], r_g.at[j], (jnp.maximum(stage - 1, 0), data))

    def partial(kind, src, dst, j):
        return rc(src.at[j, theirs], dst.at[j], s_p.at[kind, j], r_p.at[kind, j], partner)

    def enter(kind, buf, allr, j):
        share(kind, buf, j).start()
        for o in range(1, nchip):
            spread(kind, buf, allr, j, o).start()
        share(kind, buf, j).wait_recv()
        own(kind, buf, allr, j).start()

    def fwd(j):
        @pl.when(stage > 0)
        def _():
            hand_up(j).wait_recv()

        enter(0, hbuf, hall, j)

        @pl.when(j == 0)
        def _():
            for c in wcopies:
                c.wait()

        h = hbuf[j]
        for i, (f0, fw) in enumerate(tiles):
            u = mm(h, w1[:, f0:f0 + fw], ((1,), (0,)))
            ubuf[j, :, f0:f0 + fw] = u
            p = mm(gelu(u), w2[f0:f0 + fw, :], ((1,), (0,)))
            if i == 0:
                pf[j] = p
            else:
                pf[j] += p
        partial(0, pf, rf, j).start()
        partial(0, pf, rf, j).wait_recv()
        out = (hbuf[j, mine, :].astype(F32) + (pf[j, mine, :] + rf[j])).astype(BF16)

        @pl.when(stage < last)
        def _():
            hsend[j] = out
            hand_up(j).start()

        @pl.when(stage == last)
        def _():
            resid = out.astype(F32) - yv[j].astype(F32)
            gbuf[j, mine, :] = (resid / total).astype(BF16)
            loss_ref[...] += jnp.sum(resid * resid).reshape(1, 1)

    def bwd(j):
        @pl.when(stage < last)
        def _():
            hand_down(j).wait_recv()

        enter(1, gbuf, gall, j)

        @pl.when(stage > 0)
        def _():
            g = gbuf[j]
            for i, (f0, fw) in enumerate(tiles):
                e = mm(g, w2[f0:f0 + fw, :], ((1,), (1,)))
                q = (e * gelu_grad(ubuf[j, :, f0:f0 + fw])).astype(BF16)
                p = mm(q, w1[:, f0:f0 + fw], ((1,), (1,)))
                if i == 0:
                    pb[j] = p
                else:
                    pb[j] += p
            partial(1, pb, rb, j).start()
            partial(1, pb, rb, j).wait_recv()
            gsend[j] = (gbuf[j, mine, :].astype(F32) + (pb[j, mine, :] + rb[j])).astype(BF16)
            hand_down(j).start()

    is_last = jnp.where(stage == last, 1, 0)

    def step(t, carry):
        j = is_last * (t // 2) + (1 - is_last) * (t % nc)
        back = is_last * (t % 2) + (1 - is_last) * (t // nc)

        @pl.when(back == 0)
        def _():
            fwd(j)

        @pl.when(back == 1)
        def _():
            bwd(j)

        return carry

    lax.fori_loop(0, 2 * nc, step, 0)

    kinds = ((0, hbuf, hall), (1, gbuf, gall))
    for kind, buf, allr in kinds:
        for j in range(nc):
            for o in range(1, nchip):
                arrived(kind, buf, allr, j, o).wait_recv()
                forward(kind, allr, j, o).start()
    for kind, buf, allr in kinds:
        for j in range(nc):
            own(kind, buf, allr, j).wait()
            share(kind, buf, j).wait_send()
            for o in range(1, nchip):
                spread(kind, buf, allr, j, o).wait_send()
                forward(kind, allr, j, o).wait_send()
                rc(allr.at[(chip + nchip - o) % nchip, j, theirs], allr.at[(chip + nchip - o) % nchip, j, theirs],
                   s_f.at[kind, j, o], r_f.at[kind, j, o], partner).wait_recv()
    for j in range(nc):
        partial(0, pf, rf, j).wait_send()

    @pl.when(stage > 0)
    def _():
        for j in range(nc):
            partial(1, pb, rb, j).wait_send()
            hand_down(j).wait_send()

    @pl.when(stage < last)
    def _():
        for j in range(nc):
            hand_up(j).wait_send()


def run_chain(tokens_in, targets, w_up, w_down, n_stages, n_data):
    nc, rows, dim = tokens_in.shape
    half = w_up.shape[2] // 2
    nchip = n_data // 2
    total = nc * rows * n_data
    any_spec = pl.BlockSpec(memory_space=pl.ANY)
    dma = pltpu.SemaphoreType.DMA
    return pl.pallas_call(
        functools.partial(chain_kernel, n_stages, total),
        out_shape=(
            jax.ShapeDtypeStruct((nchip, nc, 2 * rows, dim), BF16),
            jax.ShapeDtypeStruct((nchip, nc, 2 * rows, dim), BF16),
            jax.ShapeDtypeStruct((8, 128), F32),
        ),
        in_specs=[any_spec] * 4,
        out_specs=(any_spec, any_spec, pl.BlockSpec(memory_space=pltpu.VMEM)),
        scratch_shapes=[
            pltpu.VMEM((dim, half), BF16),
            pltpu.VMEM((half, dim), BF16),
            pltpu.VMEM((nc, 2 * rows, dim), BF16),
            pltpu.VMEM((nc, 2 * rows, dim), BF16),
            pltpu.VMEM((nc, 2 * rows, half), F32),
            pltpu.VMEM((nc, 2 * rows, dim), F32),
            pltpu.VMEM((nc, 2 * rows, dim), F32),
            pltpu.VMEM((nc, rows, dim), F32),
            pltpu.VMEM((nc, rows, dim), F32),
            pltpu.VMEM((nc, rows, dim), BF16),
            pltpu.VMEM((nc, rows, dim), BF16),
            pltpu.VMEM((nc, rows, dim), BF16),
            dma((2,)), dma((nc,)), dma((nc,)), dma((nc,)), dma((nc,)), dma((nc,)),
            dma((2, nc)), dma((2, nc)), dma((2, nc)), dma((2, nc)),
            dma((2, nc, nchip)), dma((2, nc, nchip)), dma((2, nc, nchip)), dma((2, nc, nchip)),
        ],
        compiler_params=pltpu.CompilerParams(has_side_effects=True, vmem_limit_bytes=67043328),
        name="chain",
    )(tokens_in, targets, w_up, w_down)


TILE = 1280
TOKENS = 512


def grad_kernel(n_stages, hall, gall, w1_ref, w2_ref, loss_ref, up_o, down_o, stat_o,
                hv, gv, ht, gt, w1b, w2b, upa, upx, dna, dnx, red1, red2, red3,
                s_in, s_w, s_o, s_s, r_s, s_r, r_r):
    stage = lax.axis_index("stage")
    data = lax.axis_index("data")
    chip, core = data // 2, data % 2
    total, dim = hv.shape
    part, half = upa.shape
    nchip = red2.shape[0]
    partner = (stage, chip * 2 + (1 - core))
    foff = pl.multiple_of(core * half, 128)
    mine = pl.ds(pl.multiple_of(core * part, 16), part)
    theirs = pl.ds(pl.multiple_of((1 - core) * part, 16), part)
    n_full, tail = half // TILE, half % TILE
    n_tiles = n_full + (1 if tail else 0)

    def rc(src, dst, ss, rs, dev):
        return pltpu.make_async_remote_copy(
            src_ref=src, dst_ref=dst, send_sem=ss, recv_sem=rs, device_id=dev, device_id_type=MESH)

    def loads(i, fw):
        slot = i % 2
        src = pl.ds(pl.multiple_of(foff + i * TILE, 128), fw)
        return (
            pltpu.make_async_copy(w1_ref.at[0, :, src], w1b.at[slot, :, pl.ds(0, fw)], s_w.at[slot, 0]),
            pltpu.make_async_copy(w2_ref.at[0, src, :], w2b.at[slot, pl.ds(0, fw), :], s_w.at[slot, 1]),
        )

    def start_load(i, fw):
        for c in loads(i, fw):
            c.start()

    load_h = pltpu.make_async_copy(hall, hv, s_in.at[0])
    load_g = pltpu.make_async_copy(gall, gv, s_in.at[1])
    load_h.start()
    load_g.start()
    start_load(0, TILE)
    stat_o[0] = jnp.zeros((8, 128), F32)
    stat_o[1] = loss_ref[...]
    cols = pl.ds(pl.multiple_of(chip * (2 * part), 128), 2 * part)
    load_h.wait()
    load_g.wait()
    for c in range(total // TOKENS):
        r = slice(c * TOKENS, (c + 1) * TOKENS)
        ht[:, r] = hv[r, cols].T
        gt[:, r] = gv[r, cols].T

    def outs(i, fw):
        fs = pl.ds(pl.multiple_of(i * TILE, 128), fw)
        dst = pl.ds(pl.multiple_of(foff + i * TILE, 128), fw)
        return (
            pltpu.make_async_copy(upa.at[:, fs], up_o.at[:, dst], s_o.at[i, 0]),
            pltpu.make_async_copy(dna.at[:, fs], down_o.at[:, dst], s_o.at[i, 1]),
            rc(upx.at[:, fs], up_o.at[:, dst], s_s.at[i, 0], r_s.at[i, 0], partner),
            rc(dnx.at[:, fs], down_o.at[:, dst], s_s.at[i, 1], r_s.at[i, 1], partner),
        )

    def compute(i, fw):
        slot = i % 2
        fs = pl.ds(pl.multiple_of(i * TILE, 128), fw)
        for c in loads(i, fw):
            c.wait()
        for buf in (upa, upx, dna, dnx):
            buf[:, fs] = jnp.zeros((part, fw), F32)

        def chunk(c, carry):
            r = pl.ds(pl.multiple_of(c * TOKENS, TOKENS), TOKENS)
            u = mm(hv[r, :], w1b[slot, :, :fw], ((1,), (0,)))
            e = mm(gv[r, :], w2b[slot, :fw, :], ((1,), (1,)))
            uu = u * u
            t = jnp.tanh(K0 * u * (1.0 + K1 * uu))
            cdf = 0.5 * (1.0 + t)
            a = (u * cdf).astype(BF16)
            q = (e * (cdf + (0.5 * K0) * u * (1.0 - t * t) * (1.0 + 3.0 * K1 * uu))).astype(BF16)
            dna[:, fs] += mm(gt[mine, r], a, ((1,), (0,)))
            dnx[:, fs] += mm(gt[theirs, r], a, ((1,), (0,)))
            upa[:, fs] += mm(ht[mine, r], q, ((1,), (0,)))
            upx[:, fs] += mm(ht[theirs, r], q, ((1,), (0,)))
            return carry

        lax.fori_loop(0, total // TOKENS, chunk, 0)
        for c in outs(i, fw):
            c.start()
        acc = jnp.zeros((8, fw), F32)
        for buf in (upa, upx, dna, dnx):
            v = buf[:, fs]
            acc += jnp.sum((v * v).reshape(part // 8, 8, fw), axis=0)
        sq = acc[:, :128]
        for k in range(1, fw // 128):
            sq += acc[:, k * 128:(k + 1) * 128]
        stat_o[0] += sq

    def tile_step(i, carry):
        @pl.when(i + 1 < n_full)
        def _():
            start_load(i + 1, TILE)

        if tail:
            @pl.when(i + 1 == n_full)
            def _():
                start_load(i + 1, tail)

        compute(i, TILE)
        return carry

    lax.fori_loop(0, n_full, tile_step, 0)
    if tail:
        compute(n_full, tail)

    red1[core] = stat_o[...]
    c1 = rc(red1.at[core], red1.at[core], s_r.at[0, 0], r_r.at[0, 0], partner)
    c1.start()
    c1.wait()
    red2[chip] = red1[0] + red1[1]

    def to_chip(o):
        return rc(red2.at[chip], red2.at[chip], s_r.at[1, o], r_r.at[1, o],
                  (stage, ((chip + o) % nchip) * 2 + core))

    def to_stage(o):
        return rc(red3.at[stage], red3.at[stage], s_r.at[2, o], r_r.at[2, o], ((stage + o) % n_stages, data))

    for o in range(1, nchip):
        to_chip(o).start()
    for o in range(1, nchip):
        to_chip(o).wait()
    v = red2[0]
    for k in range(1, nchip):
        v = v + red2[k]
    red3[stage] = v
    for o in range(1, n_stages):
        to_stage(o).start()
    for o in range(1, n_stages):
        to_stage(o).wait()
    v = red3[0]
    for k in range(1, n_stages):
        v = v + red3[k]
    stat_o[...] = v
    for i in range(n_tiles):
        for c in outs(i, TILE if i < n_full else tail):
            c.wait()


def run_grads(h_all, g_all, w_up, w_down, loss, n_stages, n_data):
    total, dim = h_all.shape
    ffn = w_up.shape[2]
    half = ffn // 2
    part = dim // n_data
    nchip = n_data // 2
    n_tiles = -(-half // TILE)
    any_spec = pl.BlockSpec(memory_space=pl.ANY)
    vmem = pl.BlockSpec(memory_space=pltpu.VMEM)
    dma = pltpu.SemaphoreType.DMA
    peers = max(nchip, n_stages)
    return pl.pallas_call(
        functools.partial(grad_kernel, n_stages),
        out_shape=(
            jax.ShapeDtypeStruct((part, ffn), F32),
            jax.ShapeDtypeStruct((part, ffn), F32),
            jax.ShapeDtypeStruct((2, 8, 128), F32),
        ),
        in_specs=[any_spec] * 4 + [vmem],
        out_specs=(any_spec, any_spec, vmem),
        scratch_shapes=[
            pltpu.VMEM((total, dim), BF16),
            pltpu.VMEM((total, dim), BF16),
            pltpu.VMEM((2 * part, total), BF16),
            pltpu.VMEM((2 * part, total), BF16),
            pltpu.VMEM((2, dim, TILE), BF16),
            pltpu.VMEM((2, TILE, dim), BF16),
            pltpu.VMEM((part, half), F32),
            pltpu.VMEM((part, half), F32),
            pltpu.VMEM((part, half), F32),
            pltpu.VMEM((part, half), F32),
            pltpu.VMEM((2, 2, 8, 128), F32),
            pltpu.VMEM((nchip, 2, 8, 128), F32),
            pltpu.VMEM((n_stages, 2, 8, 128), F32),
            dma((2,)), dma((2, 2)), dma((n_tiles, 2)), dma((n_tiles, 2)), dma((n_tiles, 2)),
            dma((3, peers)), dma((3, peers)),
        ],
        compiler_params=pltpu.CompilerParams(has_side_effects=True, vmem_limit_bytes=67043328),
        name="grads",
    )(h_all, g_all, w_up, w_down, loss)


def solution(mesh):
    n_stages = mesh.shape["stage"]
    n_data = mesh.shape["data"]

    def device_step(tokens_in, targets, w_up, w_down, clip_norm):
        n_micro, n_tokens, dim = tokens_in.shape
        total = n_micro * n_tokens * n_data
        h_all, g_all, loss = run_chain(tokens_in, targets, w_up, w_down, n_stages, n_data)
        up, down, stat = run_grads(h_all.reshape(total, dim), g_all.reshape(total, dim), w_up, w_down, loss,
                                   n_stages, n_data)
        scale = jnp.minimum(1.0, clip_norm / jnp.sqrt(jnp.sum(stat[0])))
        return stat[1, 0, 0] / (2 * total), (up * scale)[None], (down * scale).T[None]

    return jax.shard_map(
        device_step,
        mesh=mesh,
        in_specs=(P("data"), P("data"), P("stage"), P("stage"), P()),
        out_specs=(P(), P("stage", "data", None), P("stage", None, "data")),
        check_vma=False,
    )
```
